128 devices in a mesh: dp: 1, b: 64 (over z, y, x), cp: 2 (over core).
Axes of the slice: x: 4, y: 4, z: 4, core: 2. Of those that a mesh axis runs over, the one named last changes fastest.
Arguments:
- x: bfloat16 [64, 256, 2048], P(('dp', 'b'), 'cp')
- ids: int32 [64, 256, 12], P(('dp', 'b'), 'cp')
- g_attn: bfloat16 [2048], replicated
- wq: bfloat16 [2048, 4096], replicated
- wk: bfloat16 [2048, 512], replicated
- wv: bfloat16 [2048, 512], replicated
- wo: bfloat16 [4096, 2048], replicated
- g_ffn: bfloat16 [2048], replicated
- w1: bfloat16 [2048, 6144], replicated
- w3: bfloat16 [2048, 6144], replicated
- w2: bfloat16 [6144, 2048], replicated
- g_moe: bfloat16 [2048], replicated
- wr: bfloat16 [2048, 192], replicated
- we_g: bfloat16 [128, 2048, 768], P(('b', 'cp'))
- we_u: bfloat16 [128, 2048, 768], P(('b', 'cp'))
- we_d: bfloat16 [128, 768, 2048], P(('b', 'cp'))
Outputs:
- output: bfloat16 [64, 256, 2048], P(('dp', 'b'), 'cp')
All inputs are finite; a program needn't handle non-finite values.
Results may differ from the reference program's by a relative error of at most 0.00847203.
Values are sent between devices in bfloat16 or wider.
A program may use at most 1 GiB of HBM per device.

```python
import jax
import jax.numpy as jnp
from jax import lax

BATCH = 64
SEQ = 256
D = 2048
HEADS = 32
KV_HEADS = 4
FF = 6144
EFF = 768
EXPERTS = 128
ZERO = 64
TOP = 12
NB = 64
NC = 2
HEAD = 128
ROPE = 64
QB = 64
EPS = 1e-6
THETA = 10000.0
RSCALE = 2.5


def rms_norm(x, g):
    xf = x.astype(jnp.float32)
    r = lax.rsqrt(jnp.mean(xf * xf, axis=-1, keepdims=True) + EPS)
    return (xf * r * g.astype(jnp.float32)).astype(jnp.bfloat16)


def rope(t, pos):
    half = ROPE // 2
    freq = THETA ** (-jnp.arange(half, dtype=jnp.float32) / half)
    ang = pos.astype(jnp.float32)[:, None] * freq[None, :]
    c = jnp.cos(ang)[:, None, :]
    s = jnp.sin(ang)[:, None, :]
    tf = t.astype(jnp.float32)
    t1 = tf[..., :half]
    t2 = tf[..., half:ROPE]
    out = jnp.concatenate([t1 * c - t2 * s, t2 * c + t1 * s, tf[..., ROPE:]], axis=-1)
    return out.astype(jnp.bfloat16)


def slot_rank(key):
    n = key.shape[0]
    order = jnp.argsort(key, stable=True)
    sk = key[order]
    first = jnp.searchsorted(sk, sk)
    return jnp.zeros((n,), jnp.int32).at[order].set((jnp.arange(n) - first).astype(jnp.int32))


def setup_inputs(seed: int = 0, part: int = 0) -> dict:
    kg = jax.random.key(seed)
    ks = jax.random.split(kg, 16)
    kp = jax.random.split(jax.random.fold_in(kg, part), 8)
    kz = jax.random.fold_in(kg, 7919)
    kzs = jax.random.split(kz, 2)
    kr = jax.random.split(jax.random.fold_in(kz, part + 1), 4)
    bd = BATCH // NB
    sd = SEQ // NC
    tl = bd * sd
    ns = tl * TOP
    cap = tl * TOP // EXPERTS
    nblk = NB * NC
    nseg = 16

    def w(k, shape, fan, sc):
        return (jax.random.normal(k, shape, jnp.float32) * (sc * fan ** -0.5)).astype(jnp.bfloat16)

    def gain(k):
        return (1.0 + 0.25 * jax.random.normal(k, (D,), jnp.float32)).astype(jnp.bfloat16)

    seg = jnp.arange(SEQ) * nseg // SEQ
    zs = jax.random.normal(kp[0], (BATCH, nseg, D), jnp.float32)
    noise = jax.random.normal(kp[1], (BATCH, SEQ, D), jnp.float32)
    x = (0.8 * zs[:, seg, :] + 0.6 * noise).astype(jnp.bfloat16)

    def limit(raw, zid):
        ffn = raw < EXPERTS
        rank = slot_rank(jnp.where(ffn, raw, EXPERTS))
        return jnp.where(ffn & (rank < cap), raw, zid)

    pop_sum = jnp.sum(jax.random.randint(kzs[0], (EXPERTS, 12), 0, 256), axis=1)
    pop_exp = jnp.clip((pop_sum - 1536) * 277 // 4096 + 64, 0, 127)
    pop_weight = (8 + (pop_exp & 7)) << (pop_exp >> 3)
    pop_cum = jnp.cumsum(pop_weight).astype(jnp.int32)
    zero_limit = jax.random.randint(kr[0], (nblk, tl, 1), 3277, 45876)
    zero_bits = (jax.random.bits(kr[1], (nblk, tl, TOP), jnp.uint32) >> 16).astype(jnp.int32)
    zero_pick = (zero_bits < zero_limit).reshape(nblk, ns)
    pick_draw = jax.random.randint(kr[2], (nblk, ns), 0, pop_cum[-1])
    ffn_id = jnp.minimum(jnp.searchsorted(pop_cum, pick_draw, side='right'), EXPERTS - 1).astype(jnp.int32)
    zero_id = EXPERTS + jax.random.randint(kr[3], (nblk, ns), 0, max(ZERO // 4, 1))
    raw = jnp.where(zero_pick, EXPERTS, ffn_id)
    blk = jax.vmap(limit)(raw, zero_id).astype(jnp.int32)
    ids = blk.reshape(NB, NC, bd, sd, TOP).transpose(0, 2, 1, 3, 4).reshape(BATCH, SEQ, TOP)
    return {
        'x': x,
        'ids': ids,
        'g_attn': gain(ks[0]),
        'wq': w(ks[1], (D, HEADS * HEAD), D, 2.0),
        'wk': w(ks[2], (D, KV_HEADS * HEAD), D, 1.0),
        'wv': w(ks[3], (D, KV_HEADS * HEAD), D, 1.0),
        'wo': w(ks[4], (HEADS * HEAD, D), HEADS * HEAD, 1.0),
        'g_ffn': gain(ks[5]),
        'w1': w(ks[6], (D, FF), D, 1.0),
        'w3': w(ks[7], (D, FF), D, 1.0),
        'w2': w(ks[8], (FF, D), FF, 1.0),
        'g_moe': gain(ks[9]),
        'wr': w(ks[10], (D, EXPERTS + ZERO), D, 1.5),
        'we_g': w(ks[11], (EXPERTS, D, EFF), D, 1.0),
        'we_u': w(ks[12], (EXPERTS, D, EFF), D, 1.0),
        'we_d': w(ks[13], (EXPERTS, EFF, D), EFF, 1.0),
    }


def reference(x, ids, g_attn, wq, wk, wv, wo, g_ffn, w1, w3, w2, g_moe, wr, we_g, we_u, we_d):
    S = x.shape[1]
    pos = jnp.arange(S)
    grp = HEADS // KV_HEADS
    scale = HEAD ** -0.5

    def proj(a, wt):
        return jnp.dot(a, wt, preferred_element_type=jnp.float32).astype(jnp.bfloat16)

    def attn_row(xr):
        n = rms_norm(xr, g_attn)
        q = rope(proj(n, wq).reshape(S, HEADS, HEAD), pos).reshape(S, KV_HEADS, grp, HEAD).astype(jnp.float32)
        k = rope(proj(n, wk).reshape(S, KV_HEADS, HEAD), pos).astype(jnp.float32)
        v = proj(n, wv).reshape(S, KV_HEADS, HEAD).astype(jnp.float32)

        def qblock(i):
            qb = lax.dynamic_slice_in_dim(q, i * QB, QB, axis=0)
            sc = jnp.einsum('qkgd,skd->kgqs', qb, k) * scale
            qp = i * QB + jnp.arange(QB)
            sc = jnp.where(qp[:, None] >= pos[None, :], sc, -jnp.inf)
            p = jax.nn.softmax(sc, axis=-1)
            return jnp.einsum('kgqs,skd->qkgd', p, v)

        o = lax.map(qblock, jnp.arange(S // QB)).reshape(S, HEADS * HEAD).astype(jnp.bfloat16)
        return proj(o, wo)

    a = lax.map(attn_row, x)
    y = (x.astype(jnp.float32) + a.astype(jnp.float32)).astype(jnp.bfloat16)

    def ffn_row(yr):
        z = rms_norm(yr, g_ffn)
        hh = (jax.nn.silu(jnp.dot(z, w1, preferred_element_type=jnp.float32)) * jnp.dot(z, w3, preferred_element_type=jnp.float32)).astype(jnp.bfloat16)
        return proj(hh, w2)

    f = lax.map(ffn_row, y)

    nt = BATCH * S
    N = nt * TOP
    gcap = N // EXPERTS
    u = rms_norm(x, g_moe).reshape(nt, D)
    logits = jnp.dot(u, wr, preferred_element_type=jnp.float32)
    idf = ids.reshape(nt, TOP)
    gate = RSCALE * jax.nn.softmax(jnp.take_along_axis(logits, idf, axis=1), axis=-1)
    e = idf.reshape(N)
    ffn = e < EXPERTS
    ek = jnp.where(ffn, e, EXPERTS)
    slot = jnp.where(ffn, ek * gcap + slot_rank(ek), EXPERTS * gcap)
    us = u[jnp.arange(N) // TOP]
    buf = jnp.zeros((EXPERTS * gcap, D), jnp.bfloat16).at[slot].set(us, mode='drop')

    def expert(args):
        xb, a1, a2, a3 = args
        hh = (jax.nn.silu(jnp.dot(xb, a1, preferred_element_type=jnp.float32)) * jnp.dot(xb, a2, preferred_element_type=jnp.float32)).astype(jnp.bfloat16)
        return proj(hh, a3)

    out = lax.map(expert, (buf.reshape(EXPERTS, gcap, D), we_g, we_u, we_d)).reshape(EXPERTS * gcap, D)
    got = out[jnp.minimum(slot, EXPERTS * gcap - 1)]
    val = jnp.where(ffn[:, None], got.astype(jnp.float32), us.astype(jnp.float32)).reshape(nt, TOP, D)
    m = jnp.einsum('tj,tjd->td', gate, val)
    h = y.astype(jnp.float32) + f.astype(jnp.float32) + m.reshape(BATCH, S, D)
    return h.astype(jnp.bfloat16)
```

```python
import jax
import jax.numpy as jnp
from jax import lax
from jax.experimental import pallas as pl
from jax.experimental.pallas import tpu as pltpu
from jax.sharding import PartitionSpec as P

HEAD = 128
ROPE = 64
EPS = 1e-6
THETA = 10000.0
RSCALE = 2.5
F32 = jnp.float32
BF16 = jnp.bfloat16


def rms_norm(x, g):
    xf = x.astype(F32)
    r = lax.rsqrt(jnp.mean(xf * xf, axis=-1, keepdims=True) + EPS)
    return (xf * r * g.astype(F32)).astype(BF16)


def rope(t, pos):
    half = ROPE // 2
    freq = THETA ** (-jnp.arange(half, dtype=F32) / half)
    ang = pos.astype(F32)[:, None] * freq[None, :]
    c = jnp.cos(ang)[:, None, :]
    s = jnp.sin(ang)[:, None, :]
    tf = t.astype(F32)
    t1 = tf[..., :half]
    t2 = tf[..., half:ROPE]
    out = jnp.concatenate([t1 * c - t2 * s, t2 * c + t1 * s, tf[..., ROPE:]], axis=-1)
    return out.astype(BF16)


def proj(a, wt):
    return jnp.dot(a, wt, preferred_element_type=F32).astype(BF16)


def swiglu(z, wa, wb, wc):
    hh = (jax.nn.silu(jnp.dot(z, wa, preferred_element_type=F32)) * jnp.dot(z, wb, preferred_element_type=F32)).astype(BF16)
    return proj(hh, wc)


def nt(a, b):
    return lax.dot_general(a, b, (((1,), (1,)), ((), ())), preferred_element_type=F32)


def nn(a, b):
    return jnp.dot(a, b, preferred_element_type=F32)


def count(ids, base, width):
    t, top = ids.shape
    lane = lax.broadcasted_iota(jnp.int32, (t, width), 1) + base
    c = jnp.zeros((t, width), F32)
    for j in range(top):
        c = c + jnp.where(ids[:, j:j + 1] == lane, 1.0, 0.0)
    return c


def dispatch_kernel(c_ref, xa_ref, xb_ref, ia_ref, ib_ref, g_ref, send_ref, u_ref, first_ref, last_ref, *, cap, rows):
    t = xa_ref.shape[0]
    nexp = first_ref.shape[1]

    @pl.when(pl.program_id(0) == 0)
    def _():
        g = g_ref[...].astype(F32)
        ti = lax.broadcasted_iota(jnp.int32, (t, t), 0)
        tj = lax.broadcasted_iota(jnp.int32, (t, t), 1)
        lower = jnp.where(tj < ti, 1.0, 0.0).astype(BF16)
        for k, (x_ref, i_ref) in enumerate(((xa_ref, ia_ref), (xb_ref, ib_ref))):
            xf = x_ref[...].astype(F32)
            r = lax.rsqrt(jnp.mean(xf * xf, axis=-1, keepdims=True) + EPS)
            u_ref[k * t:(k + 1) * t, :] = (xf * r * g).astype(BF16)
            cnt = count(i_ref[...], 0, nexp)
            excl = nn(lower, cnt.astype(BF16))
            first_ref[k * t:(k + 1) * t, :] = excl
            last_ref[k * t:(k + 1) * t, :] = excl + cnt

    base = pl.program_id(0) * rows
    row = (lax.broadcasted_iota(jnp.int32, (rows, nexp), 0) + base).astype(F32)
    col = lax.broadcasted_iota(jnp.int32, (rows, nexp), 1)
    own = jnp.floor((row + 0.5) * (1.0 / (2 * cap))).astype(jnp.int32)
    pick = jnp.where(col == 2 * own + c_ref[0], 1.0, 0.0).astype(BF16)
    lo = nt(pick, first_ref[...].astype(BF16))
    hi = nt(pick, last_ref[...].astype(BF16))
    rw = (lax.broadcasted_iota(jnp.int32, (rows, 2 * t), 0) + base).astype(F32)
    tok = lax.broadcasted_iota(jnp.int32, (rows, 2 * t), 1)
    rr = rw - (2 * cap) * jnp.floor((rw + 0.5) * (1.0 / (2 * cap))) - jnp.where(tok >= t, float(cap), 0.0)
    sel = jnp.where((lo <= rr) & (rr < hi), 1.0, 0.0).astype(BF16)
    send_ref[...] = nn(sel, u_ref[...]).astype(BF16)


def dispatch(c, xa, xb, ia, ib, g, cap, nexp):
    t, d = xa.shape
    top = ia.shape[1]
    n = nexp * cap
    nblk = 4
    rows = n // nblk
    full = lambda shape: pl.BlockSpec(shape, lambda i: (0, 0))
    import functools
    return pl.pallas_call(
        functools.partial(dispatch_kernel, cap=cap, rows=rows),
        grid=(nblk,),
        in_specs=[pl.BlockSpec(memory_space=pltpu.SMEM), full((t, d)), full((t, d)), full((t, top)), full((t, top)), full((1, d))],
        out_specs=[pl.BlockSpec((rows, d), lambda i: (i, 0)), full((2 * t, d)), full((2 * t, nexp)), full((2 * t, nexp))],
        out_shape=[
            jax.ShapeDtypeStruct((n, d), BF16),
            jax.ShapeDtypeStruct((2 * t, d), BF16),
            jax.ShapeDtypeStruct((2 * t, nexp), F32),
            jax.ShapeDtypeStruct((2 * t, nexp), F32),
        ],
        compiler_params=pltpu.CompilerParams(dimension_semantics=("arbitrary",)),
        cost_estimate=pl.CostEstimate(flops=2 * n * 2 * t * d, bytes_accessed=2 * n * d, transcendentals=0),
        name="dispatch",
    )(c, xa, xb, ia, ib, g)


def gates_kernel(c_ref, u_ref, ia_ref, ib_ref, wr_ref, first_ref, last_ref, g_ref, gz_ref, part_ref, *, cap, cols):
    t = ia_ref.shape[0]
    nexp = first_ref.shape[1]
    nz = wr_ref.shape[1] - nexp

    @pl.when(pl.program_id(0) == 0)
    def _():
        logits = nn(u_ref[...], wr_ref[...])
        le = logits[:, :nexp]
        lz = logits[:, nexp:]
        ce = last_ref[...] - first_ref[...]
        cz = jnp.concatenate([count(ia_ref[...], nexp, nz), count(ib_ref[...], nexp, nz)], axis=0)
        mx = jnp.maximum(
            jnp.max(jnp.where(ce > 0, le, -jnp.inf), axis=-1, keepdims=True),
            jnp.max(jnp.where(cz > 0, lz, -jnp.inf), axis=-1, keepdims=True),
        )
        xe = jnp.where(ce > 0, jnp.exp(le - mx), 0.0)
        xz = jnp.where(cz > 0, jnp.exp(lz - mx), 0.0)
        sz = jnp.sum(cz * xz, axis=-1, keepdims=True)
        den = jnp.sum(ce * xe, axis=-1, keepdims=True) + sz
        gate = RSCALE * (xe / den)
        gz_ref[...] = jnp.broadcast_to(RSCALE * (sz / den), gz_ref.shape)
        hi = gate.astype(BF16)
        r1 = gate - hi.astype(F32)
        mid = r1.astype(BF16)
        r2 = r1 - mid.astype(F32)
        part_ref[0:2 * t, :] = hi
        part_ref[2 * t:4 * t, :] = mid
        part_ref[4 * t:6 * t, :] = r2.astype(BF16)

    base = pl.program_id(0) * cols
    row = lax.broadcasted_iota(jnp.int32, (nexp, cols), 0)
    col = (lax.broadcasted_iota(jnp.int32, (nexp, cols), 1) + base).astype(F32)
    own = jnp.floor((col + 0.5) * (1.0 / (2 * cap))).astype(jnp.int32)
    pick = jnp.where(row == 2 * own + c_ref[0], 1.0, 0.0).astype(BF16)
    lo = nn(first_ref[...].astype(BF16), pick)
    hi = nn(last_ref[...].astype(BF16), pick)
    cw = (lax.broadcasted_iota(jnp.int32, (2 * t, cols), 1) + base).astype(F32)
    tok = lax.broadcasted_iota(jnp.int32, (2 * t, cols), 0)
    rr = cw - (2 * cap) * jnp.floor((cw + 0.5) * (1.0 / (2 * cap))) - jnp.where(tok >= t, float(cap), 0.0)
    sel = (lo <= rr) & (rr < hi)
    for k in range(3):
        ex = nn(part_ref[k * 2 * t:(k + 1) * 2 * t, :], pick)
        g_ref[k * 2 * t:(k + 1) * 2 * t, :] = jnp.where(sel, ex, 0.0).astype(BF16)


def gates(c, u, ia, ib, wr, first, last, cap):
    t, top = ia.shape
    d = u.shape[1]
    nexp = first.shape[1]
    n = nexp * cap
    nblk = 4
    cols = n // nblk
    full = lambda shape: pl.BlockSpec(shape, lambda i: (0, 0))
    import functools
    return pl.pallas_call(
        functools.partial(gates_kernel, cap=cap, cols=cols),
        grid=(nblk,),
        in_specs=[pl.BlockSpec(memory_space=pltpu.SMEM), full((2 * t, d)), full((t, top)), full((t, top)), full(wr.shape), full((2 * t, nexp)), full((2 * t, nexp))],
        out_specs=[pl.BlockSpec((6 * t, cols), lambda i: (0, i)), full((2 * t, 128))],
        out_shape=[jax.ShapeDtypeStruct((6 * t, n), BF16), jax.ShapeDtypeStruct((2 * t, 128), F32)],
        scratch_shapes=[pltpu.VMEM((6 * t, nexp), BF16)],
        compiler_params=pltpu.CompilerParams(dimension_semantics=("arbitrary",)),
        cost_estimate=pl.CostEstimate(flops=2 * 2 * t * d * wr.shape[1] + 10 * 2 * t * nexp * n, bytes_accessed=12 * t * n, transcendentals=2 * t * wr.shape[1]),
        name="gates",
    )(c, u, ia, ib, wr, first, last)


def combine_kernel(g_ref, back_ref, u_ref, gz_ref, own_ref, oth_ref):
    t = own_ref.shape[0]
    acc = nn(g_ref[...], back_ref[...])
    m = acc[0:2 * t] + (acc[2 * t:4 * t] + acc[4 * t:6 * t])
    own_ref[...] = m[:t] + gz_ref[0:t, 0:1] * u_ref[...].astype(F32)
    oth_ref[...] = m[t:]


def combine(g, back, u, gz, t):
    n, d = back.shape
    blk = 512
    return pl.pallas_call(
        combine_kernel,
        grid=(d // blk,),
        in_specs=[
            pl.BlockSpec(g.shape, lambda i: (0, 0)),
            pl.BlockSpec((n, blk), lambda i: (0, i)),
            pl.BlockSpec((t, blk), lambda i: (0, i)),
            pl.BlockSpec(gz.shape, lambda i: (0, 0)),
        ],
        out_specs=[pl.BlockSpec((t, blk), lambda i: (0, i)), pl.BlockSpec((t, blk), lambda i: (0, i))],
        out_shape=[jax.ShapeDtypeStruct((t, d), F32), jax.ShapeDtypeStruct((t, d), F32)],
        compiler_params=pltpu.CompilerParams(dimension_semantics=("arbitrary",)),
        cost_estimate=pl.CostEstimate(flops=2 * g.shape[0] * n * d, bytes_accessed=2 * n * d, transcendentals=0),
        name="combine",
    )(g, back, u, gz)


def solution(mesh):
    ncp = mesh.shape['cp']
    nb = mesh.shape['b']
    tok = P(('dp', 'b'), 'cp', None)
    rep = P()
    exs = P(('b', 'cp'), None, None)
    swap = [(0, 1), (1, 0)]

    def body(x, ids, g_attn, wq, wk, wv, wo, g_ffn, w1, w3, w2, g_moe, wr, we_g, we_u, we_d):
        bd, sd, d = x.shape
        top = ids.shape[-1]
        nh = wq.shape[1] // HEAD
        kvh = wk.shape[1] // HEAD
        grp = nh // kvh
        nexp = nb * ncp
        cap = sd * top // nexp
        ci = lax.axis_index('cp')
        cs = ci.astype(jnp.int32).reshape(1)

        xa = x.reshape(sd, d)
        ia = ids.reshape(sd, top)
        xb = lax.ppermute(xa, 'cp', swap)
        ib = lax.ppermute(ia, 'cp', swap)

        send, u2, first, last = dispatch(cs, xa, xb, ia, ib, g_moe.reshape(1, d), cap, nexp)
        recv = lax.all_to_all(send.reshape(nb, 2 * cap, d), 'b', 0, 0, tiled=True)

        pa = ci * sd + jnp.arange(sd)
        pb = (1 - ci) * sd + jnp.arange(sd)
        pos = jnp.concatenate([pa, pb])
        n2 = rms_norm(jnp.concatenate([xa, xb], axis=0), g_attn)
        q = rope(proj(n2[:sd], wq).reshape(sd, nh, HEAD), pa).reshape(sd, kvh, grp, HEAD).transpose(1, 2, 0, 3)
        k = rope(proj(n2, wk).reshape(2 * sd, kvh, HEAD), pos)
        v = proj(n2, wv).reshape(2 * sd, kvh, HEAD)
        s = jnp.einsum('kgqd,skd->kgqs', q, k, preferred_element_type=F32) * (HEAD ** -0.5)
        s = jnp.where(pa[:, None] >= pos[None, :], s, -1e30)
        mx = jnp.max(s, axis=-1, keepdims=True)
        p = jnp.exp(s - mx)
        den = jnp.sum(p, axis=-1)
        acc = jnp.einsum('kgqs,skd->kgqd', p.astype(BF16), v, preferred_element_type=F32)
        o = (acc / den[..., None]).astype(BF16).transpose(2, 0, 1, 3).reshape(sd, nh * HEAD)

        gall, gz = gates(cs, u2, ia, ib, wr, first, last, cap)

        xin = recv.reshape(nexp * cap, d)
        hg = nn(xin, we_g[0])
        hu = nn(xin, we_u[0])
        hh = (jax.nn.silu(hg) * hu).astype(BF16)
        yo = proj(hh, we_d[0])
        back = lax.all_to_all(yo.reshape(nb, 2 * cap, d), 'b', 0, 0, tiled=True)

        y = (xa.astype(F32) + proj(o, wo).astype(F32)).astype(BF16)
        f = swiglu(rms_norm(y, g_ffn), w1, w3, w2)
        y, f = lax.optimization_barrier((y, f))

        mine, other = combine(gall, back.reshape(nexp * cap, d), u2[:sd], gz, sd)
        m = mine + lax.ppermute(other, 'cp', swap)
        h = y.astype(F32) + f.astype(F32) + m
        return h.astype(BF16).reshape(bd, sd, d)

    return jax.shard_map(body, mesh=mesh, in_specs=(tok, tok, rep, rep, rep, rep, rep, rep, rep, rep, rep, rep, rep, exs, exs, exs), out_specs=tok, check_vma=False)
```
